32 devices in a mesh: blk: 16 (over z, y, x), row: 2 (over core).
Axes of the slice: x: 2, y: 2, z: 4, core: 2. Of those that a mesh axis runs over, the one named last changes fastest.
Arguments:
- genotypes: bfloat16 [128, 16, 2048], P('blk', None, 'row'), may hold values from 0 to 2
- assignment: int32 [16], replicated, may hold values from 0 to 15, each once
- snp_counts: int32 [16], replicated, may hold values from 1024 to 2048, as said below
- basis: float32 [16, 64, 2048], P('blk', None, 'row'), may hold values from -6 to 6
Outputs:
- image: float32 [16, 64, 2048], P('blk', None, 'row')
- new_basis: float32 [16, 64, 2048], P('blk', None, 'row')
- factor: float32 [16, 64, 64], P('blk')
The draws below stay inside these ranges and needn't reach their ends.
Inputs may be any that keep to these rules, and one draw needn't show every extreme that they name: `assignment`: each block number appears exactly once. `snp_counts`: A block's SNPs fill its leading slots.
All inputs are finite; a program needn't handle non-finite values.
Results may differ from the reference program's by a relative error of at most 0.0021.
Values may be sent and summed in bfloat16 or wider, within the bound.
No kernel may reach another device: no remote copies, remote signals or barrier semaphores. Data moves between devices by JAX's collectives and lax.ppermute only.
A program may use at most 64 MiB of HBM per device.

```python
import jax
import jax.numpy as jnp
from jax import lax

BS = 2048
RANK = 64
SAMPLES = 128
BLOCKS = 16


def draw_snp_counts(key, part):
    return jax.random.randint(key, (BLOCKS,), BS // 2, BS + 1).astype(jnp.int32)


def level_of(rng, shape, cuts, least, top_value):
    factor_of, own = 1.0, jax.random.fold_in(rng, 6)
    for dim, shards_of in cuts:
        steps = jnp.exp(jax.random.uniform(jax.random.fold_in(own, dim), (shards_of,), jnp.float32, least / len(cuts), top_value / len(cuts)))
        factor_of = factor_of * jnp.repeat(steps, shape[dim] // shards_of).reshape([-1 if axis == dim else 1 for axis in range(len(shape))])
    return factor_of


def bell_draw(rng, dims, width, bound, split=(), held_as=jnp.bfloat16):
    values = width * jax.random.normal(rng, dims, jnp.float32)
    if split:
        values = values * level_of(rng, dims, split, -0.22, 0.18)
    return jnp.clip(values, -bound, bound).astype(held_as)


def setup_inputs(seed: int = 0) -> dict:
    seeds = jax.random.split(jax.random.key(seed), 5)
    genotypes = jnp.clip(2.0 * jax.random.uniform(seeds[0], (SAMPLES, BLOCKS, BS), jnp.float32) ** level_of(seeds[0], (SAMPLES, BLOCKS, BS), ((0, 16), (2, 2)), -0.2, 0.2), 0.0, 2.0).astype(jnp.bfloat16)
    assignment = jax.random.permutation(seeds[1], BLOCKS).astype(jnp.int32)
    snp_counts = draw_snp_counts(jax.random.fold_in(seeds[4], 71), 0)
    basis = bell_draw(seeds[3], (BLOCKS, RANK, BS), 1.0, 6.0, ((0, 16), (2, 2)), jnp.float32)
    return {"genotypes": genotypes, "assignment": assignment, "snp_counts": snp_counts, "basis": basis}


epsilon = 1e-05
shrink_weight = 0.5

def reference(genotypes, assignment, snp_counts, basis):
    positions = jnp.arange(BS, dtype=jnp.int32)

    def per_slot(slot_idx):
        block_id = assignment[slot_idx]
        dosage = lax.dynamic_index_in_dim(genotypes, block_id, 1, keepdims=False).astype(jnp.float32)
        live_mask = positions < snp_counts[block_id]
        col_mean = lax.optimization_barrier(jnp.mean(dosage, axis=0))
        centered = dosage - col_mean[None, :]
        col_var = lax.optimization_barrier(jnp.mean(centered * centered, axis=0))
        standard = jnp.where(live_mask[None, :], centered * lax.rsqrt(col_var + epsilon)[None, :], 0.0).astype(jnp.bfloat16)
        standard_f = standard.astype(jnp.float32)
        start_basis = basis[slot_idx]
        projected = jnp.dot(standard_f, start_basis.T, precision=lax.Precision.HIGHEST)
        product = jnp.dot(projected.T, standard_f, precision=lax.Precision.HIGHEST) / SAMPLES
        image = shrink_weight * product + (1.0 - shrink_weight) * jnp.where(live_mask[None, :], start_basis, 0.0)
        gram_sum = jnp.dot(image, image.T, precision=lax.Precision.HIGHEST)
        factor = jnp.linalg.cholesky(gram_sum)
        new_basis = jax.scipy.linalg.solve_triangular(factor, image, lower=True)
        return (image, new_basis, factor)
    image, new_basis, factor = lax.map(per_slot, jnp.arange(BLOCKS, dtype=jnp.int32))
    return (image, new_basis, factor)
```

```python
import functools

import jax
import jax.numpy as jnp
from jax import lax
from jax.experimental import pallas as pl
from jax.experimental.pallas import tpu as pltpu
from jax.sharding import PartitionSpec as P

epsilon = 1e-05
shrink_weight = 0.5

VMEM = pltpu.VMEM
SMEM = pltpu.SMEM
HIGHEST = lax.Precision.HIGHEST
f32 = jnp.float32
bf16 = jnp.bfloat16


def dot(x, y, dims, precision=None):
    return lax.dot_general(x, y, (dims, ((), ())), precision=precision, preferred_element_type=f32)


NN = ((1,), (0,))
NT = ((1,), (1,))


def in_vmem(n):
    return [pl.BlockSpec(memory_space=VMEM)] * n


def split3(x):
    high = x.astype(bf16)
    rest = x - high.astype(f32)
    mid = rest.astype(bf16)
    low = (rest - mid.astype(f32)).astype(bf16)
    return high, mid, low


def order_kernel(samples, blocks, group, assignment, rows_ref, out_ref):
    shape = (samples, samples * blocks)
    column = lax.broadcasted_iota(jnp.int32, shape, 1)
    start = lax.broadcasted_iota(jnp.int32, shape, 0) * blocks
    for first in range(0, blocks, group):
        picks = [
            jnp.where(column == start + assignment[first + s], 1.0, 0.0).astype(f32)
            for s in range(group)
        ]
        pick = jnp.concatenate(picks, axis=0).astype(bf16)
        out_ref[first * samples : (first + group) * samples, :] = dot(
            pick, rows_ref[...], NN
        ).astype(bf16)


def basis_kernel(half, assignment, snp_counts, basis_ref, split_ref, masked_ref, live_ref, gram_ref):
    count = snp_counts[assignment[lax.axis_index("blk")]]
    basis = basis_ref[...]
    rank = basis.shape[0]
    column = lax.broadcasted_iota(jnp.int32, (8, half), 1) + lax.axis_index("row") * half
    live = jnp.where(column < count, 1.0, 0.0).astype(f32)
    live_ref[...] = live
    masked = basis * live[:1]
    masked_ref[...] = masked * (1.0 - shrink_weight)
    for i, piece in enumerate(split3(basis)):
        split_ref[i * rank : (i + 1) * rank, :] = piece
    gram_ref[...] = dot(masked, masked, NT, HIGHEST)


def project_kernel(rank, values_ref, live_ref, split_ref, standard_ref, part_ref):
    values = values_ref[...].astype(f32)
    samples = values.shape[0]
    mean = jnp.sum(values, axis=0, keepdims=True) * (1.0 / samples)
    centered = values - mean
    var = jnp.sum(centered * centered, axis=0, keepdims=True) * (1.0 / samples)
    scale = lax.rsqrt(var + epsilon)
    standard = jnp.where(live_ref[:1] > 0.0, centered * scale, 0.0).astype(bf16)
    standard_ref[...] = standard
    wide = dot(split_ref[...], standard, NT)
    part_ref[:rank, :] = wide[:rank] + (wide[rank : 2 * rank] + wide[2 * rank :])
    part_ref[rank:, :] = dot(standard, standard, NT)


def factor_and_inverse(gram, panel):
    rank = gram.shape[0]
    eye = jnp.where(
        lax.broadcasted_iota(jnp.int32, (rank, rank), 0)
        == lax.broadcasted_iota(jnp.int32, (rank, rank), 1),
        1.0,
        0.0,
    ).astype(f32)
    full = jnp.concatenate([gram, eye], axis=1)
    lanes = 2 * rank
    tiles = rank // 8
    work = [full[8 * t : 8 * t + 8] for t in range(tiles)]
    sublane = lax.broadcasted_iota(jnp.int32, (8, lanes), 0)
    lane = lax.broadcasted_iota(jnp.int32, (8, lanes), 1)
    lower = [jnp.zeros((8, lanes), f32) for _ in range(tiles)]

    def row(tile, r):
        return jnp.broadcast_to(tile[r : r + 1, :], (8, lanes))

    for first in range(0, rank, panel):
        base = first // 8
        cols = [
            [
                jnp.broadcast_to(work[t][:, first + j : first + j + 1], (8, lanes))
                for t in range(base, tiles)
            ]
            for j in range(panel)
        ]
        for j in range(panel):
            k = first + j
            t0, r = k // 8, k % 8
            col = cols[j]
            root = lax.rsqrt(row(col[t0 - base], r))
            low = [c * root for c in col[t0 - base :]]
            low[0] = jnp.where(sublane >= r, low[0], 0.0)
            mult = [c * root for c in low]
            mult[0] = jnp.where(sublane > r, mult[0], 0.0)
            for j2 in range(j + 1, panel):
                other = cols[j2]
                pivot = row(other[t0 - base], r)
                for t in range(t0, tiles):
                    other[t - base] = other[t - base] - mult[t - t0] * pivot
            pivot = row(work[t0], r)
            for t in range(t0, tiles):
                work[t] = work[t] - mult[t - t0] * pivot
                lower[t] = jnp.where(lane == k, low[t - t0], lower[t])
            work[t0] = jnp.where(sublane == r, pivot * root, work[t0])
    lower = jnp.concatenate(lower, axis=0)[:, :rank]
    inverse = jnp.concatenate(work, axis=0)[:, rank:]
    return lower, inverse


def finish_kernel(
    scale, own_ref, peer_ref, own_gram_ref, peer_gram_ref, standard_ref, masked_ref,
    image_ref, new_ref, factor_ref, image_buf, new_buf, sems,
):
    rank = masked_ref.shape[0]
    total = own_ref[...] + peer_ref[...]
    proj = total[:rank]
    cross = total[rank:]
    samples = cross.shape[0]
    keep = 1.0 - shrink_weight
    diagonal = lax.broadcasted_iota(jnp.int32, (samples, samples), 0) == lax.broadcasted_iota(
        jnp.int32, (samples, samples), 1
    )
    middle = cross * (scale * scale) + jnp.where(diagonal, 2.0 * scale * keep, 0.0).astype(f32)
    gram = dot(dot(proj, middle, NN, HIGHEST), proj, NT, HIGHEST)
    gram = gram + (own_gram_ref[...] + peer_gram_ref[...]) * (keep * keep)
    rows = jnp.concatenate(split3(proj * scale), axis=0)
    wide = dot(rows, standard_ref[...], NN)
    image = wide[:rank] + (wide[rank : 2 * rank] + wide[2 * rank :]) + masked_ref[...]
    image_buf[...] = image
    image_copy = pltpu.make_async_copy(image_buf, image_ref, sems.at[0])
    image_copy.start()
    lower, inverse = factor_and_inverse(gram, 8)
    factor_ref[...] = lower
    new_buf[...] = dot(inverse, image, NN, HIGHEST)
    new_copy = pltpu.make_async_copy(new_buf, new_ref, sems.at[1])
    new_copy.start()
    image_copy.wait()
    new_copy.wait()


def body(genotypes, assignment, snp_counts, basis):
    samples, blocks, half = genotypes.shape
    owned, rank, _ = basis.shape
    assert owned == 1
    group = 16 if blocks % 16 == 0 else blocks
    scalars = [pl.BlockSpec(memory_space=SMEM)]
    ordered = pl.pallas_call(
        functools.partial(order_kernel, samples, blocks, group),
        out_shape=jax.ShapeDtypeStruct((blocks * samples, half), bf16),
        in_specs=scalars + in_vmem(1),
        out_specs=pl.BlockSpec(memory_space=VMEM),
        name="order",
    )(assignment, genotypes.reshape(samples * blocks, half))
    regrouped = lax.all_to_all(
        ordered.reshape(blocks, samples, half), "blk", split_axis=0, concat_axis=0, tiled=True
    )
    split, masked, live, basis_gram = pl.pallas_call(
        functools.partial(basis_kernel, half),
        out_shape=[
            jax.ShapeDtypeStruct((3 * rank, half), bf16),
            jax.ShapeDtypeStruct((rank, half), f32),
            jax.ShapeDtypeStruct((8, half), f32),
            jax.ShapeDtypeStruct((rank, rank), f32),
        ],
        in_specs=scalars * 2 + in_vmem(1),
        out_specs=in_vmem(4),
        cost_estimate=pl.CostEstimate(flops=2**26, bytes_accessed=2**20, transcendentals=0),
        name="basis",
    )(assignment, snp_counts, basis[0])
    swap = [(0, 1), (1, 0)]
    peer_basis_gram = lax.ppermute(basis_gram, "row", swap)
    total = blocks * samples
    standard, part = pl.pallas_call(
        functools.partial(project_kernel, rank),
        out_shape=[
            jax.ShapeDtypeStruct((total, half), bf16),
            jax.ShapeDtypeStruct((rank + total, total), f32),
        ],
        in_specs=in_vmem(3),
        out_specs=in_vmem(2),
        name="project",
    )(regrouped.reshape(total, half), live, split)
    peer_part = lax.ppermute(part, "row", swap)
    image, new_basis, factor = pl.pallas_call(
        functools.partial(finish_kernel, shrink_weight / total),
        out_shape=[
            jax.ShapeDtypeStruct((rank, half), f32),
            jax.ShapeDtypeStruct((rank, half), f32),
            jax.ShapeDtypeStruct((rank, rank), f32),
        ],
        in_specs=in_vmem(6),
        out_specs=[pl.BlockSpec(memory_space=pl.ANY)] * 2 + in_vmem(1),
        scratch_shapes=[
            pltpu.VMEM((rank, half), f32),
            pltpu.VMEM((rank, half), f32),
            pltpu.SemaphoreType.DMA((2,)),
        ],
        name="finish",
    )(part, peer_part, basis_gram, peer_basis_gram, standard, masked)
    return image[None], new_basis[None], factor[None]


def solution(mesh):
    in_specs = (P("blk", None, "row"), P(), P(), P("blk", None, "row"))
    out_specs = (P("blk", None, "row"), P("blk", None, "row"), P("blk", None, None))
    return jax.shard_map(body, mesh=mesh, in_specs=in_specs, out_specs=out_specs, check_vma=False)
```

```python
import functools

import jax
import jax.numpy as jnp
from jax import lax
from jax.experimental import pallas as pl
from jax.experimental.pallas import tpu as pltpu
from jax.sharding import PartitionSpec as P

epsilon = 1e-05
WIDTH = 256
PANELS = tuple((f, f, f + 8) for f in range(0, 64, 8))
shrink_weight = 0.5

VMEM = pltpu.VMEM
SMEM = pltpu.SMEM
HIGHEST = lax.Precision.HIGHEST
f32 = jnp.float32
bf16 = jnp.bfloat16


def dot(x, y, dims, precision=None):
    return lax.dot_general(x, y, (dims, ((), ())), precision=precision, preferred_element_type=f32)


NN = ((1,), (0,))
NT = ((1,), (1,))


def in_vmem(n):
    return [pl.BlockSpec(memory_space=VMEM)] * n


def split3(x):
    high = x.astype(bf16)
    rest = x - high.astype(f32)
    mid = rest.astype(bf16)
    low = (rest - mid.astype(f32)).astype(bf16)
    return high, mid, low


def order_kernel(
    samples, blocks, group, width, assignment_ref, rows_ref, out_ref,
    assignment, rows, ordered, scalar_sem, in_sems, out_sems,
):
    pieces = rows_ref.shape[1] // width
    fetch = pltpu.make_async_copy(assignment_ref, assignment, scalar_sem)
    fetch.start()
    loads, stores = [], []
    for i in range(pieces):
        columns = pl.ds(i * width, width)
        loads.append(
            pltpu.make_async_copy(rows_ref.at[:, columns], rows.at[:, columns], in_sems.at[i])
        )
        stores.append(
            pltpu.make_async_copy(ordered.at[:, columns], out_ref.at[:, columns], out_sems.at[i])
        )
        loads[i].start()
    shape = (samples, samples * blocks)
    column = lax.broadcasted_iota(jnp.int32, shape, 1)
    start = lax.broadcasted_iota(jnp.int32, shape, 0) * blocks
    fetch.wait()
    picks = []
    for first in range(0, blocks, group):
        ones = [
            jnp.where(column == start + assignment[first + s], 1.0, 0.0).astype(f32)
            for s in range(group)
        ]
        picks.append(jnp.concatenate(ones, axis=0).astype(bf16))
    for i in range(pieces):
        loads[i].wait()
        columns = slice(i * width, (i + 1) * width)
        for g, pick in enumerate(picks):
            span = slice(g * group * samples, (g + 1) * group * samples)
            ordered[span, columns] = dot(pick, rows[:, columns], NN).astype(bf16)
        stores[i].start()
    for store in stores:
        store.wait()


def basis_kernel(half, assignment, snp_counts, basis_ref, split_ref, masked_ref, live_ref, gram_ref):
    count = snp_counts[assignment[lax.axis_index("blk")]]
    basis = basis_ref[...]
    rank = basis.shape[0]
    column = lax.broadcasted_iota(jnp.int32, (8, half), 1) + lax.axis_index("row") * half
    live = jnp.where(column < count, 1.0, 0.0).astype(f32)
    live_ref[...] = live
    masked = basis * live[:1]
    masked_ref[...] = masked * (1.0 - shrink_weight)
    for i, piece in enumerate(split3(basis)):
        split_ref[i * rank : (i + 1) * rank, :] = piece
    gram_ref[...] = dot(masked, masked, NT, HIGHEST)


def project_kernel(
    rank, values_ref, live_ref, split_ref, own_gram_ref, peer_gram_ref,
    standard_ref, part_ref, gram_ref,
):
    values = values_ref[...].astype(f32)
    samples = values.shape[0]
    mean = jnp.sum(values, axis=0, keepdims=True) * (1.0 / samples)
    centered = values - mean
    var = jnp.sum(centered * centered, axis=0, keepdims=True) * (1.0 / samples)
    scale = lax.rsqrt(var + epsilon)
    standard = jnp.where(live_ref[:1] > 0.0, centered * scale, 0.0).astype(bf16)
    standard_ref[...] = standard
    wide = dot(split_ref[...], standard, NT)
    part_ref[:rank, :] = wide[:rank] + (wide[rank : 2 * rank] + wide[2 * rank :])
    part_ref[rank:, :] = dot(standard, standard, NT)
    gram_ref[...] = (own_gram_ref[...] + peer_gram_ref[...]) * (1.0 - shrink_weight) ** 2


def factor_and_inverse(gram, panels):
    rank = gram.shape[0]
    row_ids = lax.broadcasted_iota(jnp.int32, (rank, rank), 0)
    col_ids = lax.broadcasted_iota(jnp.int32, (rank, rank), 1)
    eye = jnp.where(row_ids == col_ids, 1.0, 0.0).astype(f32)
    full = jnp.concatenate([gram, eye], axis=1)
    lanes = 2 * rank
    tiles = rank // 8
    work = [full[8 * t : 8 * t + 8] for t in range(tiles)]
    sublane = lax.broadcasted_iota(jnp.int32, (8, lanes), 0)
    cols = {}

    def row(tile, r):
        return jnp.broadcast_to(tile[r : r + 1, :], (8, lanes))

    for k in range(rank):
        for start, first, last in panels:
            if start == k:
                for j in range(first, last):
                    for t in range(j // 8, tiles):
                        cols[j, t] = jnp.broadcast_to(work[t][:, j : j + 1], (8, lanes))
        t0, r = k // 8, k % 8
        root = lax.rsqrt(row(cols[k, t0], r))
        square = root * root
        mult = {t: cols[k, t] * square for t in range(t0, tiles)}
        mult[t0] = jnp.where(sublane > r, mult[t0], 0.0)
        for j in range(k + 1, rank):
            if (j, tiles - 1) in cols:
                pivot = row(cols[k, j // 8], j % 8)
                for t in range(j // 8, tiles):
                    cols[j, t] = cols[j, t] - mult[t] * pivot
        pivot = row(work[t0], r)
        for t in range(t0, tiles):
            work[t] = work[t] - mult[t] * pivot
            del cols[k, t]
        work[t0] = jnp.where(sublane == r, pivot * root, work[t0])
    whole = jnp.concatenate(work, axis=0)
    upper = jnp.where(row_ids <= col_ids, whole[:, :rank], 0.0)
    return upper.T, whole[:, rank:]


def finish_kernel(
    scale, own_ref, peer_ref, basis_gram_ref, standard_ref, masked_ref,
    image_ref, new_ref, factor_ref, image_buf, new_buf, factor_buf, sems,
):
    rank = masked_ref.shape[0]
    total = own_ref[...] + peer_ref[...]
    proj = total[:rank]
    cross = total[rank:]
    samples = cross.shape[0]
    keep = 1.0 - shrink_weight
    diagonal = lax.broadcasted_iota(jnp.int32, (samples, samples), 0) == lax.broadcasted_iota(
        jnp.int32, (samples, samples), 1
    )
    middle = cross * (scale * scale) + jnp.where(diagonal, 2.0 * scale * keep, 0.0).astype(f32)
    gram = dot(dot(proj, middle, NN, HIGHEST), proj, NT, HIGHEST) + basis_gram_ref[...]
    rows = jnp.concatenate(split3(proj * scale), axis=0)
    wide = dot(rows, standard_ref[...], NN)
    image = wide[:rank] + (wide[rank : 2 * rank] + wide[2 * rank :]) + masked_ref[...]
    image_buf[...] = image
    image_copy = pltpu.make_async_copy(image_buf, image_ref, sems.at[0])
    image_copy.start()
    lower, inverse = factor_and_inverse(gram, PANELS)
    factor_buf[...] = lower
    factor_copy = pltpu.make_async_copy(factor_buf, factor_ref, sems.at[2])
    factor_copy.start()
    new_buf[...] = dot(inverse, image_buf[...], NN, HIGHEST)
    new_copy = pltpu.make_async_copy(new_buf, new_ref, sems.at[1])
    new_copy.start()
    image_copy.wait()
    factor_copy.wait()
    new_copy.wait()


def body(genotypes, assignment, snp_counts, basis):
    samples, blocks, half = genotypes.shape
    owned, rank, _ = basis.shape
    assert owned == 1
    group = 16 if blocks % 16 == 0 else blocks
    limit = 24 * 2**20
    scalars = [pl.BlockSpec(memory_space=SMEM)]
    width = min(half, WIDTH)
    pieces = half // width
    anywhere = [pl.BlockSpec(memory_space=pl.ANY)]
    ordered = pl.pallas_call(
        functools.partial(order_kernel, samples, blocks, group, width),
        out_shape=jax.ShapeDtypeStruct((blocks * samples, half), bf16),
        in_specs=anywhere * 2,
        out_specs=anywhere[0],
        scratch_shapes=[
            pltpu.SMEM((blocks,), jnp.int32),
            pltpu.VMEM((samples * blocks, half), bf16),
            pltpu.VMEM((samples * blocks, half), bf16),
            pltpu.SemaphoreType.DMA,
            pltpu.SemaphoreType.DMA((pieces,)),
            pltpu.SemaphoreType.DMA((pieces,)),
        ],
        name="order",
    )(assignment, genotypes.reshape(samples * blocks, half))
    regrouped = lax.all_to_all(
        ordered.reshape(blocks, samples, half), "blk", split_axis=0, concat_axis=0, tiled=True
    )
    split, masked, live, basis_gram = pl.pallas_call(
        functools.partial(basis_kernel, half),
        out_shape=[
            jax.ShapeDtypeStruct((3 * rank, half), bf16),
            jax.ShapeDtypeStruct((rank, half), f32),
            jax.ShapeDtypeStruct((8, half), f32),
            jax.ShapeDtypeStruct((rank, rank), f32),
        ],
        in_specs=scalars * 2 + in_vmem(1),
        out_specs=in_vmem(4),
        cost_estimate=pl.CostEstimate(flops=2**26, bytes_accessed=2**20, transcendentals=0),
        name="basis", compiler_params=pltpu.CompilerParams(vmem_limit_bytes=limit),
    )(assignment, snp_counts, basis[0])
    swap = [(0, 1), (1, 0)]
    peer_basis_gram = lax.ppermute(basis_gram, "row", swap)
    total = blocks * samples
    standard, part, gram = pl.pallas_call(
        functools.partial(project_kernel, rank),
        out_shape=[
            jax.ShapeDtypeStruct((total, half), bf16),
            jax.ShapeDtypeStruct((rank + total, total), f32),
            jax.ShapeDtypeStruct((rank, rank), f32),
        ],
        in_specs=in_vmem(5),
        out_specs=in_vmem(3),
        name="project", compiler_params=pltpu.CompilerParams(vmem_limit_bytes=limit),
    )(regrouped.reshape(total, half), live, split, basis_gram, peer_basis_gram)
    peer_part = lax.ppermute(part, "row", swap)
    image, new_basis, factor = pl.pallas_call(
        functools.partial(finish_kernel, shrink_weight / total),
        out_shape=[
            jax.ShapeDtypeStruct((rank, half), f32),
            jax.ShapeDtypeStruct((rank, half), f32),
            jax.ShapeDtypeStruct((rank, rank), f32),
        ],
        in_specs=in_vmem(5),
        out_specs=[pl.BlockSpec(memory_space=pl.ANY)] * 3,
        scratch_shapes=[
            pltpu.VMEM((rank, half), f32),
            pltpu.VMEM((rank, half), f32),
            pltpu.VMEM((rank, rank), f32),
            pltpu.SemaphoreType.DMA((3,)),
        ],
        name="finish", compiler_params=pltpu.CompilerParams(vmem_limit_bytes=limit),
    )(part, peer_part, gram, standard, masked)
    return image[None], new_basis[None], factor[None]


def solution(mesh):
    in_specs = (P("blk", None, "row"), P(), P(), P("blk", None, "row"))
    out_specs = (P("blk", None, "row"), P("blk", None, "row"), P("blk", None, None))
    return jax.shard_map(body, mesh=mesh, in_specs=in_specs, out_specs=out_specs, check_vma=False)
```

```python
import functools

import jax
import jax.numpy as jnp
from jax import lax
from jax.experimental import pallas as pl
from jax.experimental.pallas import tpu as pltpu
from jax.sharding import PartitionSpec as P

epsilon = 1e-05
PANELS = tuple((f, f, f + 8) for f in range(0, 64, 8))
shrink_weight = 0.5

VMEM = pltpu.VMEM
SMEM = pltpu.SMEM
HIGHEST = lax.Precision.HIGHEST
f32 = jnp.float32
bf16 = jnp.bfloat16


def dot(x, y, dims, precision=None):
    return lax.dot_general(x, y, (dims, ((), ())), precision=precision, preferred_element_type=f32)


NN = ((1,), (0,))
NT = ((1,), (1,))


def in_vmem(n):
    return [pl.BlockSpec(memory_space=VMEM)] * n


def split3(x):
    high = x.astype(bf16)
    rest = x - high.astype(f32)
    mid = rest.astype(bf16)
    low = (rest - mid.astype(f32)).astype(bf16)
    return high, mid, low


def order_kernel(
    samples, blocks, group, half, assignment_ref, counts_ref, rows_ref, out_ref, live_ref,
    assignment, counts, rows, sems,
):
    fetches = [
        pltpu.make_async_copy(assignment_ref, assignment, sems.at[0]),
        pltpu.make_async_copy(counts_ref, counts, sems.at[1]),
        pltpu.make_async_copy(rows_ref, rows, sems.at[2]),
    ]
    for fetch in fetches:
        fetch.start()
    shape = (samples, samples * blocks)
    column = lax.broadcasted_iota(jnp.int32, shape, 1)
    start = lax.broadcasted_iota(jnp.int32, shape, 0) * blocks
    position = lax.broadcasted_iota(jnp.int32, (8, half), 1) + lax.axis_index("row") * half
    fetches[0].wait()
    picks = []
    for first in range(0, blocks, group):
        ones = [
            jnp.where(column == start + assignment[first + s], 1.0, 0.0).astype(f32)
            for s in range(group)
        ]
        picks.append(jnp.concatenate(ones, axis=0).astype(bf16))
    fetches[1].wait()
    count = counts[assignment[lax.axis_index("blk")]]
    live_ref[...] = jnp.where(position < count, 1.0, 0.0).astype(f32)
    fetches[2].wait()
    for g, pick in enumerate(picks):
        span = slice(g * group * samples, (g + 1) * group * samples)
        out_ref[span, :] = dot(pick, rows[...], NN).astype(bf16)


def project_kernel(values_ref, live_ref, basis_ref, standard_ref, masked_ref, part_ref):
    live = live_ref[:1]
    masked = basis_ref[...] * live
    rank = masked.shape[0]
    masked_ref[...] = masked * (1.0 - shrink_weight)
    high, mid, low = split3(masked)
    values = values_ref[...].astype(f32)
    samples = values.shape[0]
    mean = jnp.sum(values, axis=0, keepdims=True) * (1.0 / samples)
    centered = values - mean
    var = jnp.sum(centered * centered, axis=0, keepdims=True) * (1.0 / samples)
    scale = lax.rsqrt(var + epsilon)
    standard = jnp.where(live > 0.0, centered * scale, 0.0).astype(bf16)
    standard_ref[...] = standard
    left = jnp.concatenate([high, mid, low, standard], axis=0)
    right = jnp.concatenate([standard, high, mid], axis=0)
    wide = dot(left, right, NT)
    part_ref[:rank, :] = wide[:rank, :samples] + (
        wide[rank : 2 * rank, :samples] + wide[2 * rank : 3 * rank, :samples]
    )
    part_ref[rank : rank + samples, :] = wide[3 * rank :, :samples]
    at_high = slice(samples, samples + rank)
    at_mid = slice(samples + rank, samples + 2 * rank)
    even = wide[:rank, at_high] + wide[rank : 2 * rank, at_mid]
    odd = wide[rank : 2 * rank, at_high] + wide[2 * rank : 3 * rank, at_high]
    part_ref[rank + samples :, : 2 * rank] = jnp.concatenate([even, odd], axis=1)


def factor_and_inverse(gram, panels):
    rank = gram.shape[0]
    row_ids = lax.broadcasted_iota(jnp.int32, (rank, rank), 0)
    col_ids = lax.broadcasted_iota(jnp.int32, (rank, rank), 1)
    eye = jnp.where(row_ids == col_ids, 1.0, 0.0).astype(f32)
    full = jnp.concatenate([gram, eye], axis=1)
    lanes = 2 * rank
    tiles = rank // 8
    work = [full[8 * t : 8 * t + 8] for t in range(tiles)]
    sublane = lax.broadcasted_iota(jnp.int32, (8, lanes), 0)
    cols = {}

    def row(tile, r):
        return jnp.broadcast_to(tile[r : r + 1, :], (8, lanes))

    for k in range(rank):
        for start, first, last in panels:
            if start == k:
                for j in range(first, last):
                    for t in range(j // 8, tiles):
                        cols[j, t] = jnp.broadcast_to(work[t][:, j : j + 1], (8, lanes))
        t0, r = k // 8, k % 8
        root = lax.rsqrt(row(cols[k, t0], r))
        square = root * root
        mult = {t: cols[k, t] * square for t in range(t0, tiles)}
        mult[t0] = jnp.where(sublane > r, mult[t0], 0.0)
        for j in range(k + 1, rank):
            if (j, tiles - 1) in cols:
                pivot = row(cols[k, j // 8], j % 8)
                for t in range(j // 8, tiles):
                    cols[j, t] = cols[j, t] - mult[t] * pivot
        pivot = row(work[t0], r)
        for t in range(t0, tiles):
            work[t] = work[t] - mult[t] * pivot
            del cols[k, t]
        work[t0] = jnp.where(sublane == r, pivot * root, work[t0])
    whole = jnp.concatenate(work, axis=0)
    upper = jnp.where(row_ids <= col_ids, whole[:, :rank], 0.0)
    return upper.T, whole[:, rank:]


def finish_kernel(
    scale, own_ref, peer_ref, standard_ref, masked_ref,
    image_ref, new_ref, factor_ref, image_buf, new_buf, factor_buf, sems,
):
    rank = masked_ref.shape[0]
    total = own_ref[...] + peer_ref[...]
    proj = total[:rank]
    samples = total.shape[1]
    cross = total[rank : rank + samples]
    even = total[rank + samples :, :rank]
    odd = total[rank + samples :, rank : 2 * rank]
    basis_gram = even + (odd + odd.T)
    keep = 1.0 - shrink_weight
    diagonal = lax.broadcasted_iota(jnp.int32, (samples, samples), 0) == lax.broadcasted_iota(
        jnp.int32, (samples, samples), 1
    )
    middle = cross * (scale * scale) + jnp.where(diagonal, 2.0 * scale * keep, 0.0).astype(f32)
    gram = dot(dot(proj, middle, NN, HIGHEST), proj, NT, HIGHEST)
    gram = gram + basis_gram * (keep * keep)
    rows = jnp.concatenate(split3(proj * scale), axis=0)
    wide = dot(rows, standard_ref[...], NN)
    image = wide[:rank] + (wide[rank : 2 * rank] + wide[2 * rank :]) + masked_ref[...]
    image_buf[...] = image
    image_copy = pltpu.make_async_copy(image_buf, image_ref, sems.at[0])
    image_copy.start()
    lower, inverse = factor_and_inverse(gram, PANELS)
    factor_buf[...] = lower
    factor_copy = pltpu.make_async_copy(factor_buf, factor_ref, sems.at[2])
    factor_copy.start()
    new_buf[...] = dot(inverse, image_buf[...], NN, HIGHEST)
    new_copy = pltpu.make_async_copy(new_buf, new_ref, sems.at[1])
    new_copy.start()
    image_copy.wait()
    factor_copy.wait()
    new_copy.wait()


def body(genotypes, assignment, snp_counts, basis):
    samples, blocks, half = genotypes.shape
    owned, rank, _ = basis.shape
    assert owned == 1
    group = 16 if blocks % 16 == 0 else blocks
    limit = 24 * 2**20
    params = pltpu.CompilerParams(vmem_limit_bytes=limit)
    anywhere = [pl.BlockSpec(memory_space=pl.ANY)]
    ordered, live = pl.pallas_call(
        functools.partial(order_kernel, samples, blocks, group, half),
        out_shape=[
            jax.ShapeDtypeStruct((blocks * samples, half), bf16),
            jax.ShapeDtypeStruct((8, half), f32),
        ],
        in_specs=[pl.BlockSpec(memory_space=pltpu.HBM)] * 3,
        out_specs=in_vmem(2),
        scratch_shapes=[
            pltpu.SMEM((blocks,), jnp.int32),
            pltpu.SMEM((blocks,), jnp.int32),
            pltpu.VMEM((samples * blocks, half), bf16),
            pltpu.SemaphoreType.DMA((3,)),
        ],
        compiler_params=params,
        name="order",
    )(*[
        pltpu.with_memory_space_constraint(x, pltpu.HBM)
        for x in (assignment, snp_counts, genotypes.reshape(samples * blocks, half))
    ])
    regrouped = lax.all_to_all(
        ordered.reshape(blocks, samples, half), "blk", split_axis=0, concat_axis=0, tiled=True
    )
    total = blocks * samples
    standard, masked, part = pl.pallas_call(
        project_kernel,
        out_shape=[
            jax.ShapeDtypeStruct((total, half), bf16),
            jax.ShapeDtypeStruct((rank, half), f32),
            jax.ShapeDtypeStruct((2 * rank + total, total), f32),
        ],
        in_specs=in_vmem(3),
        out_specs=in_vmem(3),
        compiler_params=params,
        name="project",
    )(regrouped.reshape(total, half), live, basis[0])
    peer_part = lax.ppermute(part, "row", [(0, 1), (1, 0)])
    image, new_basis, factor = pl.pallas_call(
        functools.partial(finish_kernel, shrink_weight / total),
        out_shape=[
            jax.ShapeDtypeStruct((rank, half), f32),
            jax.ShapeDtypeStruct((rank, half), f32),
            jax.ShapeDtypeStruct((rank, rank), f32),
        ],
        in_specs=in_vmem(4),
        out_specs=anywhere * 3,
        scratch_shapes=[
            pltpu.VMEM((rank, half), f32),
            pltpu.VMEM((rank, half), f32),
            pltpu.VMEM((rank, rank), f32),
            pltpu.SemaphoreType.DMA((3,)),
        ],
        compiler_params=params,
        name="finish",
    )(part, peer_part, standard, masked)
    return image[None], new_basis[None], factor[None]


def solution(mesh):
    in_specs = (P("blk", None, "row"), P(), P(), P("blk", None, "row"))
    out_specs = (P("blk", None, "row"), P("blk", None, "row"), P("blk", None, None))
    return jax.shard_map(body, mesh=mesh, in_specs=in_specs, out_specs=out_specs, check_vma=False)
```

```python
import functools

import jax
import jax.numpy as jnp
from jax import lax
from jax.experimental import pallas as pl
from jax.experimental.pallas import tpu as pltpu
from jax.sharding import PartitionSpec as P

epsilon = 1e-05
PANELS = tuple((max(f - 4, 0), f, f + 4) for f in range(0, 64, 4))
shrink_weight = 0.5

VMEM = pltpu.VMEM
SMEM = pltpu.SMEM
HIGHEST = lax.Precision.HIGHEST
f32 = jnp.float32
bf16 = jnp.bfloat16


def dot(x, y, dims, precision=None):
    return lax.dot_general(x, y, (dims, ((), ())), precision=precision, preferred_element_type=f32)


NN = ((1,), (0,))
NT = ((1,), (1,))


def in_vmem(n):
    return [pl.BlockSpec(memory_space=VMEM)] * n


def split3(x):
    high = x.astype(bf16)
    rest = x - high.astype(f32)
    mid = rest.astype(bf16)
    low = (rest - mid.astype(f32)).astype(bf16)
    return high, mid, low


def order_kernel(
    samples, blocks, group, half, assignment_ref, counts_ref, rows_ref, out_ref, live_ref,
    assignment, counts, rows, sems,
):
    fetches = [
        pltpu.make_async_copy(assignment_ref, assignment, sems.at[0]),
        pltpu.make_async_copy(counts_ref, counts, sems.at[1]),
        pltpu.make_async_copy(rows_ref, rows, sems.at[2]),
    ]
    for fetch in fetches:
        fetch.start()
    shape = (samples, samples * blocks)
    column = lax.broadcasted_iota(jnp.int32, shape, 1)
    start = lax.broadcasted_iota(jnp.int32, shape, 0) * blocks
    position = lax.broadcasted_iota(jnp.int32, (8, half), 1) + lax.axis_index("row") * half
    fetches[0].wait()
    picks = []
    for first in range(0, blocks, group):
        ones = [
            jnp.where(column == start + assignment[first + s], 1.0, 0.0).astype(f32)
            for s in range(group)
        ]
        picks.append(jnp.concatenate(ones, axis=0).astype(bf16))
    fetches[1].wait()
    count = counts[assignment[lax.axis_index("blk")]]
    live_ref[...] = jnp.where(position < count, 1.0, 0.0).astype(f32)
    fetches[2].wait()
    for g, pick in enumerate(picks):
        span = slice(g * group * samples, (g + 1) * group * samples)
        out_ref[span, :] = dot(pick, rows[...], NN).astype(bf16)


def project_kernel(values_ref, live_ref, basis_ref, standard_ref, masked_ref, part_ref):
    live = live_ref[:1]
    masked = basis_ref[...] * live
    rank = masked.shape[0]
    masked_ref[...] = masked * (1.0 - shrink_weight)
    high, mid, low = split3(masked)
    values = values_ref[...].astype(f32)
    samples = values.shape[0]
    mean = jnp.sum(values, axis=0, keepdims=True) * (1.0 / samples)
    centered = values - mean
    var = jnp.sum(centered * centered, axis=0, keepdims=True) * (1.0 / samples)
    scale = lax.rsqrt(var + epsilon)
    standard = jnp.where(live > 0.0, centered * scale, 0.0).astype(bf16)
    standard_ref[...] = standard
    left = jnp.concatenate([high, mid, low, standard], axis=0)
    right = jnp.concatenate([standard, high, mid], axis=0)
    wide = dot(left, right, NT)
    part_ref[:rank, :] = wide[:rank, :samples] + (
        wide[rank : 2 * rank, :samples] + wide[2 * rank : 3 * rank, :samples]
    )
    part_ref[rank : rank + samples, :] = wide[3 * rank :, :samples]
    at_high = slice(samples, samples + rank)
    at_mid = slice(samples + rank, samples + 2 * rank)
    even = wide[:rank, at_high] + wide[rank : 2 * rank, at_mid]
    odd = wide[rank : 2 * rank, at_high] + wide[2 * rank : 3 * rank, at_high]
    part_ref[rank + samples :, : 2 * rank] = jnp.concatenate([even, odd], axis=1)


def factor_and_inverse(gram, panels):
    rank = gram.shape[0]
    row_ids = lax.broadcasted_iota(jnp.int32, (rank, rank), 0)
    col_ids = lax.broadcasted_iota(jnp.int32, (rank, rank), 1)
    eye = jnp.where(row_ids == col_ids, 1.0, 0.0).astype(f32)
    full = jnp.concatenate([gram, eye], axis=1)
    lanes = 2 * rank
    tiles = rank // 8
    work = [full[8 * t : 8 * t + 8] for t in range(tiles)]
    sublane = lax.broadcasted_iota(jnp.int32, (8, lanes), 0)
    cols = {}

    def row(tile, r):
        return jnp.broadcast_to(tile[r : r + 1, :], (8, lanes))

    for k in range(rank):
        for start, first, last in panels:
            if start == k:
                for j in range(first, last):
                    for t in range(j // 8, tiles):
                        cols[j, t] = jnp.take_along_axis(work[t], jnp.full((8, lanes), j, jnp.int32), axis=1)
        t0, r = k // 8, k % 8
        root = lax.rsqrt(row(cols[k, t0], r))
        square = root * root
        mult = {t: cols[k, t] * square for t in range(t0, tiles)}
        mult[t0] = jnp.where(sublane > r, mult[t0], 0.0)
        for j in range(k + 1, rank):
            if (j, tiles - 1) in cols:
                pivot = row(cols[k, j // 8], j % 8)
                for t in range(j // 8, tiles):
                    cols[j, t] = cols[j, t] - mult[t] * pivot
        pivot = row(work[t0], r)
        for t in range(t0, tiles):
            work[t] = work[t] - mult[t] * pivot
            del cols[k, t]
        work[t0] = jnp.where(sublane == r, pivot * root, work[t0])
    whole = jnp.concatenate(work, axis=0)
    upper = jnp.where(row_ids <= col_ids, whole[:, :rank], 0.0)
    lane = lax.broadcasted_iota(jnp.int32, (rank, lanes), 1)
    return upper.T, jnp.where(lane >= rank, whole, 0.0)


def finish_kernel(
    scale, own_ref, peer_ref, standard_ref, masked_ref,
    image_ref, new_ref, factor_ref, image_buf, new_buf, factor_buf, stack, sems,
):
    rank = masked_ref.shape[0]
    total = own_ref[...] + peer_ref[...]
    proj = total[:rank]
    samples = total.shape[1]
    cross = total[rank : rank + samples]
    even = total[rank + samples :, :rank]
    odd = total[rank + samples :, rank : 2 * rank]
    basis_gram = even + (odd + odd.T)
    keep = 1.0 - shrink_weight
    diagonal = lax.broadcasted_iota(jnp.int32, (samples, samples), 0) == lax.broadcasted_iota(
        jnp.int32, (samples, samples), 1
    )
    middle = cross * (scale * scale) + jnp.where(diagonal, 2.0 * scale * keep, 0.0).astype(f32)
    gram = dot(dot(proj, middle, NN, HIGHEST), proj, NT, HIGHEST)
    gram = gram + basis_gram * (keep * keep)
    rows = jnp.concatenate(split3(proj * scale), axis=0)
    wide = dot(rows, standard_ref[...], NN)
    image = wide[:rank] + (wide[rank : 2 * rank] + wide[2 * rank :]) + masked_ref[...]
    image_buf[...] = image
    image_copy = pltpu.make_async_copy(image_buf, image_ref, sems.at[0])
    image_copy.start()
    high = image.astype(bf16)
    mid = (image - high.astype(f32)).astype(bf16)
    for i, piece in enumerate((high, high, high, mid)):
        stack[i * rank : (i + 1) * rank, :] = piece
    lower, inverse = factor_and_inverse(gram, PANELS)
    high = inverse.astype(bf16)
    mid = (inverse - high.astype(f32)).astype(bf16)
    left = jnp.concatenate(
        [jnp.concatenate([high, high], axis=1), jnp.concatenate([mid, mid], axis=1)], axis=0
    )
    wide = dot(left, stack[...], NN)
    new_buf[...] = wide[:rank] + wide[rank:]
    new_copy = pltpu.make_async_copy(new_buf, new_ref, sems.at[1])
    new_copy.start()
    factor_buf[...] = lower
    factor_copy = pltpu.make_async_copy(factor_buf, factor_ref, sems.at[2])
    factor_copy.start()
    image_copy.wait()
    factor_copy.wait()
    new_copy.wait()


def body(genotypes, assignment, snp_counts, basis):
    samples, blocks, half = genotypes.shape
    owned, rank, _ = basis.shape
    assert owned == 1
    group = 16 if blocks % 16 == 0 else blocks
    limit = 24 * 2**20
    params = pltpu.CompilerParams(vmem_limit_bytes=limit)
    anywhere = [pl.BlockSpec(memory_space=pl.ANY)]
    ordered, live = pl.pallas_call(
        functools.partial(order_kernel, samples, blocks, group, half),
        out_shape=[
            jax.ShapeDtypeStruct((blocks * samples, half), bf16),
            jax.ShapeDtypeStruct((8, half), f32),
        ],
        in_specs=[pl.BlockSpec(memory_space=pltpu.HBM)] * 3,
        out_specs=in_vmem(2),
        scratch_shapes=[
            pltpu.SMEM((blocks,), jnp.int32),
            pltpu.SMEM((blocks,), jnp.int32),
            pltpu.VMEM((samples * blocks, half), bf16),
            pltpu.SemaphoreType.DMA((3,)),
        ],
        compiler_params=params,
        name="order",
    )(*[
        pltpu.with_memory_space_constraint(x, pltpu.HBM)
        for x in (assignment, snp_counts, genotypes.reshape(samples * blocks, half))
    ])
    regrouped = lax.all_to_all(
        ordered.reshape(blocks, samples, half), "blk", split_axis=0, concat_axis=0, tiled=True
    )
    total = blocks * samples
    standard, masked, part = pl.pallas_call(
        project_kernel,
        out_shape=[
            jax.ShapeDtypeStruct((total, half), bf16),
            jax.ShapeDtypeStruct((rank, half), f32),
            jax.ShapeDtypeStruct((2 * rank + total, total), f32),
        ],
        in_specs=in_vmem(3),
        out_specs=in_vmem(3),
        compiler_params=params,
        name="project",
    )(regrouped.reshape(total, half), live, basis[0])
    peer_part = lax.ppermute(part, "row", [(0, 1), (1, 0)])
    image, new_basis, factor = pl.pallas_call(
        functools.partial(finish_kernel, shrink_weight / total),
        out_shape=[
            jax.ShapeDtypeStruct((rank, half), f32),
            jax.ShapeDtypeStruct((rank, half), f32),
            jax.ShapeDtypeStruct((rank, rank), f32),
        ],
        in_specs=in_vmem(4),
        out_specs=anywhere * 3,
        scratch_shapes=[
            pltpu.VMEM((rank, half), f32),
            pltpu.VMEM((rank, half), f32),
            pltpu.VMEM((rank, rank), f32),
            pltpu.VMEM((4 * rank, half), bf16),
            pltpu.SemaphoreType.DMA((3,)),
        ],
        compiler_params=params,
        name="finish",
    )(part, peer_part, standard, masked)
    return image[None], new_basis[None], factor[None]


def solution(mesh):
    in_specs = (P("blk", None, "row"), P(), P(), P("blk", None, "row"))
    out_specs = (P("blk", None, "row"), P("blk", None, "row"), P("blk", None, None))
    return jax.shard_map(body, mesh=mesh, in_specs=in_specs, out_specs=out_specs, check_vma=False)
```

```python
import functools

import jax
import jax.numpy as jnp
from jax import lax
from jax.experimental import pallas as pl
from jax.experimental.pallas import tpu as pltpu
from jax.sharding import PartitionSpec as P

epsilon = 1e-05
shrink_weight = 0.5

VMEM = pltpu.VMEM
SMEM = pltpu.SMEM
HIGHEST = lax.Precision.HIGHEST
f32 = jnp.float32
bf16 = jnp.bfloat16


def dot(x, y, dims, precision=None):
    return lax.dot_general(x, y, (dims, ((), ())), precision=precision, preferred_element_type=f32)


NN = ((1,), (0,))
NT = ((1,), (1,))


def in_vmem(n):
    return [pl.BlockSpec(memory_space=VMEM)] * n


def split3(x):
    high = x.astype(bf16)
    rest = x - high.astype(f32)
    mid = rest.astype(bf16)
    low = (rest - mid.astype(f32)).astype(bf16)
    return high, mid, low


def order_kernel(
    samples, blocks, group, half, assignment_ref, counts_ref, rows_ref, out_ref, live_ref,
    assignment, counts, rows, sems,
):
    fetches = [
        pltpu.make_async_copy(assignment_ref, assignment, sems.at[0]),
        pltpu.make_async_copy(counts_ref, counts, sems.at[1]),
        pltpu.make_async_copy(rows_ref, rows, sems.at[2]),
    ]
    for fetch in fetches:
        fetch.start()
    shape = (samples, samples * blocks)
    column = lax.broadcasted_iota(jnp.int32, shape, 1)
    start = lax.broadcasted_iota(jnp.int32, shape, 0) * blocks
    position = lax.broadcasted_iota(jnp.int32, (8, half), 1) + lax.axis_index("row") * half
    fetches[0].wait()
    picks = []
    for first in range(0, blocks, group):
        ones = [
            jnp.where(column == start + assignment[first + s], 1.0, 0.0).astype(f32)
            for s in range(group)
        ]
        picks.append(jnp.concatenate(ones, axis=0).astype(bf16))
    fetches[1].wait()
    count = counts[assignment[lax.axis_index("blk")]]
    live_ref[...] = jnp.where(position < count, 1.0, 0.0).astype(f32)
    fetches[2].wait()
    for g, pick in enumerate(picks):
        span = slice(g * group * samples, (g + 1) * group * samples)
        out_ref[span, :] = dot(pick, rows[...], NN).astype(bf16)


def project_kernel(values_ref, live_ref, basis_ref, standard_ref, masked_ref, part_ref):
    live = live_ref[:1]
    masked = basis_ref[...] * live
    rank = masked.shape[0]
    masked_ref[...] = masked * (1.0 - shrink_weight)
    high, mid, low = split3(masked)
    values = values_ref[...].astype(f32)
    samples = values.shape[0]
    mean = jnp.sum(values, axis=0, keepdims=True) * (1.0 / samples)
    centered = values - mean
    var = jnp.sum(centered * centered, axis=0, keepdims=True) * (1.0 / samples)
    scale = lax.rsqrt(var + epsilon) * live
    standard = (centered * scale).astype(bf16)
    standard_ref[...] = standard
    left = jnp.concatenate([high, mid, low, standard], axis=0)
    right = jnp.concatenate([standard, high, mid], axis=0)
    wide = dot(left, right, NT)
    part_ref[:rank, :] = wide[:rank, :samples] + (
        wide[rank : 2 * rank, :samples] + wide[2 * rank : 3 * rank, :samples]
    )
    part_ref[rank : rank + samples, :] = wide[3 * rank :, :samples]
    at_high = slice(samples, samples + rank)
    at_mid = slice(samples + rank, samples + 2 * rank)
    even = wide[:rank, at_high] + wide[rank : 2 * rank, at_mid]
    odd = wide[rank : 2 * rank, at_high] + wide[2 * rank : 3 * rank, at_high]
    part_ref[rank + samples :, : 2 * rank] = jnp.concatenate([even, odd], axis=1)


def factor_and_inverse(gram):
    rank = gram.shape[0]
    group = 2
    panels = [
        (max(first - (4 if first < rank // 2 else 6), 0), first, first + group)
        for first in range(0, rank, group)
    ]
    row_ids = lax.broadcasted_iota(jnp.int32, (rank, rank), 0)
    col_ids = lax.broadcasted_iota(jnp.int32, (rank, rank), 1)
    eye = jnp.where(row_ids == col_ids, 1.0, 0.0).astype(f32)
    full = jnp.concatenate([gram, eye], axis=1)
    lanes = 2 * rank
    tiles = rank // 8
    work = [full[8 * t : 8 * t + 8] for t in range(tiles)]
    sublane = lax.broadcasted_iota(jnp.int32, (8, lanes), 0)
    cols = {}

    def row(tile, r):
        return jnp.broadcast_to(tile[r : r + 1, :], (8, lanes))

    diagonal = None
    for k in range(rank):
        for start, first, last in panels:
            if start == k:
                for j in range(first, last):
                    for t in range(j // 8, tiles):
                        cols[j, t] = jnp.take_along_axis(
                            work[t], jnp.full((8, lanes), j, jnp.int32), axis=1
                        )
        t0, r = k // 8, k % 8
        if k == 0:
            diagonal = row(cols[0, 0], 0)
        root = lax.rsqrt(diagonal)
        square = root * root
        if k + 1 < rank:
            t1, r1 = (k + 1) // 8, (k + 1) % 8
            side = row(cols[k, t1], r1)
            diagonal = row(cols[k + 1, t1], r1) - side * side * square
        mult = {t: cols[k, t] * square for t in range(t0, tiles)}
        for j in range(k + 1, rank):
            if (j, tiles - 1) in cols:
                pivot = row(cols[k, j // 8], j % 8)
                for t in range(j // 8, tiles):
                    cols[j, t] = cols[j, t] - mult[t] * pivot
        mult[t0] = jnp.where(sublane > r, mult[t0], 0.0)
        pivot = row(work[t0], r)
        for t in range(t0, tiles):
            work[t] = work[t] - mult[t] * pivot
            del cols[k, t]
        work[t0] = jnp.where(sublane == r, pivot * root, work[t0])
    whole = jnp.concatenate(work, axis=0)
    upper = jnp.where(row_ids <= col_ids, whole[:, :rank], 0.0)
    lane = lax.broadcasted_iota(jnp.int32, (rank, lanes), 1)
    return upper.T, jnp.where(lane >= rank, whole, 0.0)


def finish_kernel(
    scale, own_ref, peer_ref, standard_ref, masked_ref,
    image_ref, new_ref, factor_ref, image_buf, new_buf, factor_buf, stack, sems,
):
    rank = masked_ref.shape[0]
    total = own_ref[...] + peer_ref[...]
    proj = total[:rank]
    samples = total.shape[1]
    cross = total[rank : rank + samples]
    even = total[rank + samples :, :rank]
    odd = total[rank + samples :, rank : 2 * rank]
    basis_gram = even + (odd + odd.T)
    keep = 1.0 - shrink_weight
    diagonal = lax.broadcasted_iota(jnp.int32, (samples, samples), 0) == lax.broadcasted_iota(
        jnp.int32, (samples, samples), 1
    )
    middle = cross * (scale * scale) + jnp.where(diagonal, 2.0 * scale * keep, 0.0).astype(f32)
    gram = dot(dot(proj, middle, NN, HIGHEST), proj, NT, HIGHEST)
    gram = gram + basis_gram * (keep * keep)
    rows = jnp.concatenate(split3(proj * scale), axis=0)
    wide = dot(rows, standard_ref[...], NN)
    image = wide[:rank] + (wide[rank : 2 * rank] + wide[2 * rank :]) + masked_ref[...]
    image_buf[...] = image
    image_copy = pltpu.make_async_copy(image_buf, image_ref, sems.at[0])
    image_copy.start()
    high = image.astype(bf16)
    mid = (image - high.astype(f32)).astype(bf16)
    for i, piece in enumerate((high, high, high, mid)):
        stack[i * rank : (i + 1) * rank, :] = piece
    lower, inverse = factor_and_inverse(gram)
    high = inverse.astype(bf16)
    mid = (inverse - high.astype(f32)).astype(bf16)
    left = jnp.concatenate(
        [jnp.concatenate([high, high], axis=1), jnp.concatenate([mid, mid], axis=1)], axis=0
    )
    new_copies = []
    parts = 2
    width = new_buf.shape[1] // parts
    for i in range(parts):
        at = pl.ds(i * width, width)
        wide = dot(left, stack[:, i * width : (i + 1) * width], NN)
        new_buf[:, i * width : (i + 1) * width] = wide[:rank] + wide[rank:]
        new_copies.append(pltpu.make_async_copy(new_buf.at[:, at], new_ref.at[:, at], sems.at[2 + i]))
        new_copies[i].start()
    factor_buf[...] = lower
    factor_copy = pltpu.make_async_copy(factor_buf, factor_ref, sems.at[1])
    factor_copy.start()
    image_copy.wait()
    factor_copy.wait()
    for copy in new_copies:
        copy.wait()


def body(genotypes, assignment, snp_counts, basis):
    samples, blocks, half = genotypes.shape
    owned, rank, _ = basis.shape
    assert owned == 1
    group = 16 if blocks % 16 == 0 else blocks
    limit = 24 * 2**20
    params = pltpu.CompilerParams(vmem_limit_bytes=limit)
    anywhere = [pl.BlockSpec(memory_space=pl.ANY)]
    ordered, live = pl.pallas_call(
        functools.partial(order_kernel, samples, blocks, group, half),
        out_shape=[
            jax.ShapeDtypeStruct((blocks * samples, half), bf16),
            jax.ShapeDtypeStruct((8, half), f32),
        ],
        in_specs=[pl.BlockSpec(memory_space=pltpu.HBM)] * 3,
        out_specs=in_vmem(2),
        scratch_shapes=[
            pltpu.SMEM((blocks,), jnp.int32),
            pltpu.SMEM((blocks,), jnp.int32),
            pltpu.VMEM((samples * blocks, half), bf16),
            pltpu.SemaphoreType.DMA((3,)),
        ],
        compiler_params=params,
        name="order",
    )(*[
        pltpu.with_memory_space_constraint(x, pltpu.HBM)
        for x in (assignment, snp_counts, genotypes.reshape(samples * blocks, half))
    ])
    regrouped = lax.all_to_all(
        ordered.reshape(blocks, samples, half), "blk", split_axis=0, concat_axis=0, tiled=True
    )
    total = blocks * samples
    standard, masked, part = pl.pallas_call(
        project_kernel,
        out_shape=[
            jax.ShapeDtypeStruct((total, half), bf16),
            jax.ShapeDtypeStruct((rank, half), f32),
            jax.ShapeDtypeStruct((2 * rank + total, total), f32),
        ],
        in_specs=in_vmem(3),
        out_specs=in_vmem(3),
        compiler_params=params,
        name="project",
    )(regrouped.reshape(total, half), live, basis[0])
    peer_part = lax.ppermute(part, "row", [(0, 1), (1, 0)])
    image, new_basis, factor = pl.pallas_call(
        functools.partial(finish_kernel, shrink_weight / total),
        out_shape=[
            jax.ShapeDtypeStruct((rank, half), f32),
            jax.ShapeDtypeStruct((rank, half), f32),
            jax.ShapeDtypeStruct((rank, rank), f32),
        ],
        in_specs=in_vmem(4),
        out_specs=anywhere * 3,
        scratch_shapes=[
            pltpu.VMEM((rank, half), f32),
            pltpu.VMEM((rank, half), f32),
            pltpu.VMEM((rank, rank), f32),
            pltpu.VMEM((4 * rank, half), bf16),
            pltpu.SemaphoreType.DMA((4,)),
        ],
        compiler_params=params,
        name="finish",
    )(part, peer_part, standard, masked)
    return image[None], new_basis[None], factor[None]


def solution(mesh):
    in_specs = (P("blk", None, "row"), P(), P(), P("blk", None, "row"))
    out_specs = (P("blk", None, "row"), P("blk", None, "row"), P("blk", None, None))
    return jax.shard_map(body, mesh=mesh, in_specs=in_specs, out_specs=out_specs, check_vma=False)
```

```python
import functools

import jax
import jax.numpy as jnp
from jax import lax
from jax.experimental import pallas as pl
from jax.experimental.pallas import tpu as pltpu
from jax.sharding import PartitionSpec as P

epsilon = 1e-05
shrink_weight = 0.5

VMEM = pltpu.VMEM
SMEM = pltpu.SMEM
HIGHEST = lax.Precision.HIGHEST
f32 = jnp.float32
bf16 = jnp.bfloat16


def dot(x, y, dims, precision=None):
    return lax.dot_general(x, y, (dims, ((), ())), precision=precision, preferred_element_type=f32)


NN = ((1,), (0,))
NT = ((1,), (1,))


def in_vmem(n):
    return [pl.BlockSpec(memory_space=VMEM)] * n


def split3(x):
    high = x.astype(bf16)
    rest = x - high.astype(f32)
    mid = rest.astype(bf16)
    low = (rest - mid.astype(f32)).astype(bf16)
    return high, mid, low


def order_kernel(
    samples, blocks, group, half, assignment_ref, counts_ref, rows_ref, out_ref, live_ref,
    assignment, counts, rows, sems,
):
    fetches = [
        pltpu.make_async_copy(assignment_ref, assignment, sems.at[0]),
        pltpu.make_async_copy(counts_ref, counts, sems.at[1]),
        pltpu.make_async_copy(rows_ref, rows, sems.at[2]),
    ]
    for fetch in fetches:
        fetch.start()
    shape = (samples, samples * blocks)
    column = lax.broadcasted_iota(jnp.int32, shape, 1)
    start = lax.broadcasted_iota(jnp.int32, shape, 0) * blocks
    position = lax.broadcasted_iota(jnp.int32, (8, half), 1) + lax.axis_index("row") * half
    fetches[0].wait()
    picks = []
    for first in range(0, blocks, group):
        ones = [
            jnp.where(column == start + assignment[first + s], 1.0, 0.0).astype(f32)
            for s in range(group)
        ]
        picks.append(jnp.concatenate(ones, axis=0).astype(bf16))
    fetches[1].wait()
    count = counts[assignment[lax.axis_index("blk")]]
    live_ref[...] = jnp.where(position < count, 1.0, 0.0).astype(f32)
    fetches[2].wait()
    for g, pick in enumerate(picks):
        span = slice(g * group * samples, (g + 1) * group * samples)
        out_ref[span, :] = dot(pick, rows[...], NN).astype(bf16)


def project_kernel(values_ref, live_ref, basis_ref, standard_ref, masked_ref, part_ref):
    live = live_ref[:1]
    masked = basis_ref[...] * live
    rank = masked.shape[0]
    masked_ref[...] = masked * (1.0 - shrink_weight)
    high, mid, low = split3(masked)
    values = values_ref[...].astype(f32)
    samples = values.shape[0]
    mean = jnp.sum(values, axis=0, keepdims=True) * (1.0 / samples)
    centered = values - mean
    var = jnp.sum(centered * centered, axis=0, keepdims=True) * (1.0 / samples)
    scale = lax.rsqrt(var + epsilon) * live
    standard = (centered * scale).astype(bf16)
    standard_ref[...] = standard
    left = jnp.concatenate([high, mid, low, standard], axis=0)
    right = jnp.concatenate([standard, high, mid], axis=0)
    wide = dot(left, right, NT)
    part_ref[:rank, :] = wide[:rank, :samples] + (
        wide[rank : 2 * rank, :samples] + wide[2 * rank : 3 * rank, :samples]
    )
    part_ref[rank : rank + samples, :] = wide[3 * rank :, :samples]
    at_high = slice(samples, samples + rank)
    at_mid = slice(samples + rank, samples + 2 * rank)
    even = wide[:rank, at_high] + wide[rank : 2 * rank, at_mid]
    odd = wide[rank : 2 * rank, at_high] + wide[2 * rank : 3 * rank, at_high]
    part_ref[rank + samples :, : 2 * rank] = jnp.concatenate([even, odd], axis=1)


def factor_and_inverse(gram):
    rank = gram.shape[0]
    group = 2
    panels = [
        (max(first - (4 if first < rank // 2 else 6), 0), first, first + group)
        for first in range(0, rank, group)
    ]
    row_ids = lax.broadcasted_iota(jnp.int32, (rank, rank), 0)
    col_ids = lax.broadcasted_iota(jnp.int32, (rank, rank), 1)
    eye = jnp.where(row_ids == col_ids, 1.0, 0.0).astype(f32)
    full = jnp.concatenate([gram, eye], axis=1)
    lanes = 2 * rank
    tiles = rank // 8
    work = [full[8 * t : 8 * t + 8] for t in range(tiles)]
    sublane = lax.broadcasted_iota(jnp.int32, (8, lanes), 0)
    cols = {}

    def row(tile, r):
        return jnp.broadcast_to(tile[r : r + 1, :], (8, lanes))

    diagonal = None
    for k in range(rank):
        for start, first, last in panels:
            if start == k:
                for j in range(first, last):
                    for t in range(j // 8, tiles):
                        cols[j, t] = jnp.take_along_axis(
                            work[t], jnp.full((8, lanes), j, jnp.int32), axis=1
                        )
        t0, r = k // 8, k % 8
        if k == 0:
            diagonal = row(cols[0, 0], 0)
        root = lax.rsqrt(diagonal)
        square = root * root
        if k + 1 < rank:
            t1, r1 = (k + 1) // 8, (k + 1) % 8
            side = row(cols[k, t1], r1)
            diagonal = row(cols[k + 1, t1], r1) - side * side * square
        mult = {t: cols[k, t] * square for t in range(t0, tiles)}
        for j in range(k + 1, rank):
            if (j, tiles - 1) in cols:
                pivot = row(cols[k, j // 8], j % 8)
                for t in range(j // 8, tiles):
                    cols[j, t] = cols[j, t] - mult[t] * pivot
        mult[t0] = jnp.where(sublane > r, mult[t0], 0.0)
        pivot = row(work[t0], r)
        for t in range(t0, tiles):
            work[t] = work[t] - mult[t] * pivot
            del cols[k, t]
        work[t0] = jnp.where(sublane == r, pivot * root, work[t0])
    whole = jnp.concatenate(work, axis=0)
    upper = jnp.where(row_ids <= col_ids, whole[:, :rank], 0.0)
    lane = lax.broadcasted_iota(jnp.int32, (rank, lanes), 1)
    return upper.T, jnp.where(lane >= rank, whole, 0.0)


def finish_kernel(
    scale, own_ref, peer_ref, standard_ref, masked_ref,
    image_ref, new_ref, factor_ref, image_buf, new_buf, factor_buf, stack, sems,
):
    rank = masked_ref.shape[0]
    total = own_ref[...] + peer_ref[...]
    proj = total[:rank]
    samples = total.shape[1]
    cross = total[rank : rank + samples]
    even = total[rank + samples :, :rank]
    odd = total[rank + samples :, rank : 2 * rank]
    basis_gram = even + (odd + odd.T)
    keep = 1.0 - shrink_weight
    diagonal = lax.broadcasted_iota(jnp.int32, (samples, samples), 0) == lax.broadcasted_iota(
        jnp.int32, (samples, samples), 1
    )
    middle = cross * (scale * scale) + jnp.where(diagonal, 2.0 * scale * keep, 0.0).astype(f32)
    gram = dot(dot(proj, middle, NN, HIGHEST), proj, NT, HIGHEST)
    gram = gram + basis_gram * (keep * keep)
    rows = jnp.concatenate(split3(proj * scale), axis=0)
    wide = dot(rows, standard_ref[...], NN)
    image = wide[:rank] + (wide[rank : 2 * rank] + wide[2 * rank :]) + masked_ref[...]
    image_buf[...] = image
    image_copy = pltpu.make_async_copy(image_buf, image_ref, sems.at[0])
    image_copy.start()
    high = image.astype(bf16)
    mid = (image - high.astype(f32)).astype(bf16)
    for i, piece in enumerate((high, high, high, mid)):
        stack[i * rank : (i + 1) * rank, :] = piece
    lower, inverse = factor_and_inverse(gram)
    factor_buf[...] = lower
    factor_copy = pltpu.make_async_copy(factor_buf, factor_ref, sems.at[1])
    factor_copy.start()
    high = inverse.astype(bf16)
    mid = (inverse - high.astype(f32)).astype(bf16)
    left = jnp.concatenate(
        [jnp.concatenate([high, high], axis=1), jnp.concatenate([mid, mid], axis=1)], axis=0
    )
    new_copies = []
    parts = 2
    width = new_buf.shape[1] // parts
    for i in range(parts):
        at = pl.ds(i * width, width)
        wide = dot(left, stack[:, i * width : (i + 1) * width], NN)
        new_buf[:, i * width : (i + 1) * width] = wide[:rank] + wide[rank:]
        new_copies.append(pltpu.make_async_copy(new_buf.at[:, at], new_ref.at[:, at], sems.at[2 + i]))
        new_copies[i].start()
    image_copy.wait()
    factor_copy.wait()
    for copy in new_copies:
        copy.wait()


def body(genotypes, assignment, snp_counts, basis):
    samples, blocks, half = genotypes.shape
    owned, rank, _ = basis.shape
    assert owned == 1
    group = 16 if blocks % 16 == 0 else blocks
    limit = 24 * 2**20
    params = pltpu.CompilerParams(vmem_limit_bytes=limit)
    anywhere = [pl.BlockSpec(memory_space=pl.ANY)]
    ordered, live = pl.pallas_call(
        functools.partial(order_kernel, samples, blocks, group, half),
        out_shape=[
            jax.ShapeDtypeStruct((blocks * samples, half), bf16),
            jax.ShapeDtypeStruct((8, half), f32),
        ],
        in_specs=[pl.BlockSpec(memory_space=pltpu.HBM)] * 3,
        out_specs=in_vmem(2),
        scratch_shapes=[
            pltpu.SMEM((blocks,), jnp.int32),
            pltpu.SMEM((blocks,), jnp.int32),
            pltpu.VMEM((samples * blocks, half), bf16),
            pltpu.SemaphoreType.DMA((3,)),
        ],
        compiler_params=params,
        name="order",
    )(*[
        pltpu.with_memory_space_constraint(x, pltpu.HBM)
        for x in (assignment, snp_counts, genotypes.reshape(samples * blocks, half))
    ])
    regrouped = lax.all_to_all(
        ordered.reshape(blocks, samples, half), "blk", split_axis=0, concat_axis=0, tiled=True
    )
    total = blocks * samples
    standard, masked, part = pl.pallas_call(
        project_kernel,
        out_shape=[
            jax.ShapeDtypeStruct((total, half), bf16),
            jax.ShapeDtypeStruct((rank, half), f32),
            jax.ShapeDtypeStruct((2 * rank + total, total), f32),
        ],
        in_specs=in_vmem(3),
        out_specs=in_vmem(3),
        compiler_params=params,
        name="project",
    )(regrouped.reshape(total, half), live, basis[0])
    peer_part = lax.ppermute(part, "row", [(0, 1), (1, 0)])
    image, new_basis, factor = pl.pallas_call(
        functools.partial(finish_kernel, shrink_weight / total),
        out_shape=[
            jax.ShapeDtypeStruct((rank, half), f32),
            jax.ShapeDtypeStruct((rank, half), f32),
            jax.ShapeDtypeStruct((rank, rank), f32),
        ],
        in_specs=in_vmem(4),
        out_specs=anywhere * 3,
        scratch_shapes=[
            pltpu.VMEM((rank, half), f32),
            pltpu.VMEM((rank, half), f32),
            pltpu.VMEM((rank, rank), f32),
            pltpu.VMEM((4 * rank, half), bf16),
            pltpu.SemaphoreType.DMA((4,)),
        ],
        compiler_params=params,
        name="finish",
    )(part, peer_part, standard, masked)
    return image[None], new_basis[None], factor[None]


def solution(mesh):
    in_specs = (P("blk", None, "row"), P(), P(), P("blk", None, "row"))
    out_specs = (P("blk", None, "row"), P("blk", None, "row"), P("blk", None, None))
    return jax.shard_map(body, mesh=mesh, in_specs=in_specs, out_specs=out_specs, check_vma=False)
```

```python
import functools

import jax
import jax.numpy as jnp
from jax import lax
from jax.experimental import pallas as pl
from jax.experimental.pallas import tpu as pltpu
from jax.sharding import PartitionSpec as P

epsilon = 1e-05
shrink_weight = 0.5

VMEM = pltpu.VMEM
SMEM = pltpu.SMEM
HIGHEST = lax.Precision.HIGHEST
f32 = jnp.float32
bf16 = jnp.bfloat16


def dot(x, y, dims, precision=None):
    return lax.dot_general(x, y, (dims, ((), ())), precision=precision, preferred_element_type=f32)


NN = ((1,), (0,))
NT = ((1,), (1,))


def in_vmem(n):
    return [pl.BlockSpec(memory_space=VMEM)] * n


def split3(x):
    high = x.astype(bf16)
    rest = x - high.astype(f32)
    mid = rest.astype(bf16)
    low = (rest - mid.astype(f32)).astype(bf16)
    return high, mid, low


def order_kernel(
    samples, blocks, group, half, assignment_ref, counts_ref, rows_ref, out_ref, live_ref,
    assignment, counts, rows, sems,
):
    fetches = [
        pltpu.make_async_copy(assignment_ref, assignment, sems.at[0]),
        pltpu.make_async_copy(counts_ref, counts, sems.at[1]),
        pltpu.make_async_copy(rows_ref, rows, sems.at[2]),
    ]
    for fetch in fetches:
        fetch.start()
    shape = (samples, samples * blocks)
    column = lax.broadcasted_iota(jnp.int32, shape, 1)
    start = lax.broadcasted_iota(jnp.int32, shape, 0) * blocks
    position = lax.broadcasted_iota(jnp.int32, (8, half), 1) + lax.axis_index("row") * half
    fetches[0].wait()
    picks = []
    for first in range(0, blocks, group):
        ones = [
            jnp.where(column == start + assignment[first + s], 1.0, 0.0).astype(f32)
            for s in range(group)
        ]
        picks.append(jnp.concatenate(ones, axis=0).astype(bf16))
    fetches[1].wait()
    count = counts[assignment[lax.axis_index("blk")]]
    live_ref[...] = jnp.where(position < count, 1.0, 0.0).astype(f32)
    fetches[2].wait()
    for g, pick in enumerate(picks):
        span = slice(g * group * samples, (g + 1) * group * samples)
        out_ref[span, :] = dot(pick, rows[...], NN).astype(bf16)


def project_kernel(values_ref, live_ref, basis_ref, standard_ref, masked_ref, part_ref):
    live = live_ref[:1]
    masked = basis_ref[...] * live
    rank = masked.shape[0]
    masked_ref[...] = masked * (1.0 - shrink_weight)
    high, mid, low = split3(masked)
    values = values_ref[...].astype(f32)
    samples = values.shape[0]
    mean = jnp.sum(values, axis=0, keepdims=True) * (1.0 / samples)
    centered = values - mean
    var = jnp.sum(centered * centered, axis=0, keepdims=True) * (1.0 / samples)
    scale = lax.rsqrt(var + epsilon) * live
    standard = (centered * scale).astype(bf16)
    standard_ref[...] = standard
    left = jnp.concatenate([high, mid, low, standard], axis=0)
    right = jnp.concatenate([standard, high, mid], axis=0)
    wide = dot(left, right, NT)
    part_ref[:rank, :] = wide[:rank, :samples] + (
        wide[rank : 2 * rank, :samples] + wide[2 * rank : 3 * rank, :samples]
    )
    part_ref[rank : rank + samples, :] = wide[3 * rank :, :samples]
    at_high = slice(samples, samples + rank)
    at_mid = slice(samples + rank, samples + 2 * rank)
    even = wide[:rank, at_high] + wide[rank : 2 * rank, at_mid]
    odd = wide[rank : 2 * rank, at_high] + wide[2 * rank : 3 * rank, at_high]
    part_ref[rank + samples :, : 2 * rank] = jnp.concatenate([even, odd], axis=1)


def factor_and_inverse(gram):
    rank = gram.shape[0]
    group = 4
    panels = [
        (max(first - (4 if first < rank // 2 else 8), 0), first, first + group)
        for first in range(0, rank, group)
    ]
    row_ids = lax.broadcasted_iota(jnp.int32, (rank, rank), 0)
    col_ids = lax.broadcasted_iota(jnp.int32, (rank, rank), 1)
    eye = jnp.where(row_ids == col_ids, 1.0, 0.0).astype(f32)
    full = jnp.concatenate([gram, eye], axis=1)
    lanes = 2 * rank
    tiles = rank // 8
    work = [full[8 * t : 8 * t + 8] for t in range(tiles)]
    sublane = lax.broadcasted_iota(jnp.int32, (8, lanes), 0)
    cols = {}

    def row(tile, r):
        return jnp.broadcast_to(tile[r : r + 1, :], (8, lanes))

    diagonal = None
    for k in range(rank):
        for start, first, last in panels:
            if start == k:
                for j in range(first, last):
                    for t in range(j // 8, tiles):
                        cols[j, t] = jnp.take_along_axis(
                            work[t], jnp.full((8, lanes), j, jnp.int32), axis=1
                        )
        t0, r = k // 8, k % 8
        if k == 0:
            diagonal = row(cols[0, 0], 0)
        root = lax.rsqrt(diagonal)
        square = root * root
        if k + 1 < rank:
            t1, r1 = (k + 1) // 8, (k + 1) % 8
            side = row(cols[k, t1], r1)
            diagonal = row(cols[k + 1, t1], r1) - side * side * square
        mult = {t: cols[k, t] * square for t in range(t0, tiles)}
        for j in range(k + 1, rank):
            if (j, tiles - 1) in cols:
                pivot = row(cols[k, j // 8], j % 8)
                for t in range(j // 8, tiles):
                    cols[j, t] = cols[j, t] - mult[t] * pivot
        mult[t0] = jnp.where(sublane > r, mult[t0], 0.0)
        pivot = row(work[t0], r)
        for t in range(t0, tiles):
            work[t] = work[t] - mult[t] * pivot
            del cols[k, t]
        work[t0] = jnp.where(sublane == r, pivot * root, work[t0])
    whole = jnp.concatenate(work, axis=0)
    upper = jnp.where(row_ids <= col_ids, whole[:, :rank], 0.0)
    lane = lax.broadcasted_iota(jnp.int32, (rank, lanes), 1)
    return upper.T, jnp.where(lane >= rank, whole, 0.0)


def finish_kernel(
    scale, own_ref, peer_ref, standard_ref, masked_ref,
    image_ref, new_ref, factor_ref, image_buf, new_buf, factor_buf, stack, sems,
):
    rank = masked_ref.shape[0]
    total = own_ref[...] + peer_ref[...]
    proj = total[:rank]
    samples = total.shape[1]
    cross = total[rank : rank + samples]
    even = total[rank + samples :, :rank]
    odd = total[rank + samples :, rank : 2 * rank]
    basis_gram = even + (odd + odd.T)
    keep = 1.0 - shrink_weight
    diagonal = lax.broadcasted_iota(jnp.int32, (samples, samples), 0) == lax.broadcasted_iota(
        jnp.int32, (samples, samples), 1
    )
    middle = cross * (scale * scale) + jnp.where(diagonal, 2.0 * scale * keep, 0.0).astype(f32)
    gram = dot(dot(proj, middle, NN, HIGHEST), proj, NT, HIGHEST)
    gram = gram + basis_gram * (keep * keep)
    rows = jnp.concatenate(split3(proj * scale), axis=0)
    wide = dot(rows, standard_ref[...], NN)
    image = wide[:rank] + (wide[rank : 2 * rank] + wide[2 * rank :]) + masked_ref[...]
    image_buf[...] = image
    image_copy = pltpu.make_async_copy(image_buf, image_ref, sems.at[0])
    image_copy.start()
    high = image.astype(bf16)
    mid = (image - high.astype(f32)).astype(bf16)
    for i, piece in enumerate((high, high, high, mid)):
        stack[i * rank : (i + 1) * rank, :] = piece
    lower, inverse = factor_and_inverse(gram)
    factor_buf[...] = lower
    factor_copy = pltpu.make_async_copy(factor_buf, factor_ref, sems.at[1])
    factor_copy.start()
    high = inverse.astype(bf16)
    mid = (inverse - high.astype(f32)).astype(bf16)
    left = jnp.concatenate(
        [jnp.concatenate([high, high], axis=1), jnp.concatenate([mid, mid], axis=1)], axis=0
    )
    new_copies = []
    parts = 2
    width = new_buf.shape[1] // parts
    for i in range(parts):
        at = pl.ds(i * width, width)
        wide = dot(left, stack[:, i * width : (i + 1) * width], NN)
        new_buf[:, i * width : (i + 1) * width] = wide[:rank] + wide[rank:]
        new_copies.append(pltpu.make_async_copy(new_buf.at[:, at], new_ref.at[:, at], sems.at[2 + i]))
        new_copies[i].start()
    image_copy.wait()
    factor_copy.wait()
    for copy in new_copies:
        copy.wait()


def body(genotypes, assignment, snp_counts, basis):
    samples, blocks, half = genotypes.shape
    owned, rank, _ = basis.shape
    assert owned == 1
    group = 16 if blocks % 16 == 0 else blocks
    limit = 24 * 2**20
    params = pltpu.CompilerParams(vmem_limit_bytes=limit)
    anywhere = [pl.BlockSpec(memory_space=pl.ANY)]
    ordered, live = pl.pallas_call(
        functools.partial(order_kernel, samples, blocks, group, half),
        out_shape=[
            jax.ShapeDtypeStruct((blocks * samples, half), bf16),
            jax.ShapeDtypeStruct((8, half), f32),
        ],
        in_specs=[pl.BlockSpec(memory_space=pltpu.HBM)] * 3,
        out_specs=in_vmem(2),
        scratch_shapes=[
            pltpu.SMEM((blocks,), jnp.int32),
            pltpu.SMEM((blocks,), jnp.int32),
            pltpu.VMEM((samples * blocks, half), bf16),
            pltpu.SemaphoreType.DMA((3,)),
        ],
        compiler_params=params,
        name="order",
    )(*[
        pltpu.with_memory_space_constraint(x, pltpu.HBM)
        for x in (assignment, snp_counts, genotypes.reshape(samples * blocks, half))
    ])
    regrouped = lax.all_to_all(
        ordered.reshape(blocks, samples, half), "blk", split_axis=0, concat_axis=0, tiled=True
    )
    total = blocks * samples
    standard, masked, part = pl.pallas_call(
        project_kernel,
        out_shape=[
            jax.ShapeDtypeStruct((total, half), bf16),
            jax.ShapeDtypeStruct((rank, half), f32),
            jax.ShapeDtypeStruct((2 * rank + total, total), f32),
        ],
        in_specs=in_vmem(3),
        out_specs=in_vmem(3),
        compiler_params=params,
        name="project",
    )(regrouped.reshape(total, half), live, basis[0])
    peer_part = lax.ppermute(part, "row", [(0, 1), (1, 0)])
    image, new_basis, factor = pl.pallas_call(
        functools.partial(finish_kernel, shrink_weight / total),
        out_shape=[
            jax.ShapeDtypeStruct((rank, half), f32),
            jax.ShapeDtypeStruct((rank, half), f32),
            jax.ShapeDtypeStruct((rank, rank), f32),
        ],
        in_specs=in_vmem(4),
        out_specs=anywhere * 3,
        scratch_shapes=[
            pltpu.VMEM((rank, half), f32),
            pltpu.VMEM((rank, half), f32),
            pltpu.VMEM((rank, rank), f32),
            pltpu.VMEM((4 * rank, half), bf16),
            pltpu.SemaphoreType.DMA((4,)),
        ],
        compiler_params=params,
        name="finish",
    )(part, peer_part, standard, masked)
    return image[None], new_basis[None], factor[None]


def solution(mesh):
    in_specs = (P("blk", None, "row"), P(), P(), P("blk", None, "row"))
    out_specs = (P("blk", None, "row"), P("blk", None, "row"), P("blk", None, None))
    return jax.shard_map(body, mesh=mesh, in_specs=in_specs, out_specs=out_specs, check_vma=False)
```
